8 devices in a mesh: ens: 1 (over z), part: 2 (over y), feat: 4 (over x, core).
Axes of the slice: x: 2, y: 2, z: 1, core: 2. Of those that a mesh axis runs over, the one named last changes fastest.
Arguments:
- particles: float32 [4096, 2048], P(('ens', 'part'), 'feat')
- prec_diag: float32 [2048], P(('ens', 'feat'))
- target_mean: float32 [2048], P(('ens', 'feat'))
- low_factor: bfloat16 [2048, 16], P(('ens', 'feat'))
Outputs:
- output: float32 [4096, 2048], P(('ens', 'part'), 'feat')
All inputs are finite; a program needn't handle non-finite values.
Results may differ from the reference program's by a relative error of at most 0.00403875.
Values are sent between devices in bfloat16 or wider.
A program may use at most 1 GiB of HBM per device.

```python
import math
import jax
import jax.numpy as jnp

NUM_PARTICLES = 4096
FEAT_DIM = 2048
LOW_RANK = 16
NUM_STEPS = 3

KERN_WIDTH = 2.0 * FEAT_DIM / math.log(NUM_PARTICLES)
STEP_SIZE = 0.15 * NUM_PARTICLES * FEAT_DIM / math.log(NUM_PARTICLES)


def setup_inputs(seed: int = 0, part: int = 0) -> dict:
    part_key = jax.random.fold_in(jax.random.key(seed), part)
    sub_keys = jax.random.split(part_key, 6)
    scale_c = math.log(NUM_PARTICLES) / FEAT_DIM
    prec_diag = scale_c * jax.random.uniform(sub_keys[0], (FEAT_DIM,), jnp.float32, 0.5, 1.5)
    low_f32 = (math.sqrt(math.log(NUM_PARTICLES)) / FEAT_DIM) * jax.random.normal(sub_keys[1], (FEAT_DIM, LOW_RANK), jnp.float32)
    low_factor = low_f32.astype(jnp.bfloat16)
    target_mean = 0.5 * jax.random.normal(sub_keys[2], (FEAT_DIM,), jnp.float32)
    offset = 0.5 * jax.random.normal(sub_keys[3], (FEAT_DIM,), jnp.float32)
    spread = math.sqrt(0.5) * jax.random.normal(sub_keys[4], (NUM_PARTICLES, FEAT_DIM), jnp.float32)
    low_coeff = (FEAT_DIM / math.sqrt(2.0 * LOW_RANK * math.log(NUM_PARTICLES))) * jax.random.normal(sub_keys[5], (NUM_PARTICLES, LOW_RANK), jnp.float32)
    low_part = jnp.dot(low_coeff, low_factor.astype(jnp.float32).T)
    particles = target_mean[None, :] + offset[None, :] + spread + low_part
    return {"particles": particles, "prec_diag": prec_diag, "target_mean": target_mean, "low_factor": low_factor}


def svgd_step(cur_theta, prec_diag, target_mean, low_factor):
    x_dev = cur_theta - target_mean[None, :]
    proj_low = jnp.dot(x_dev.astype(jnp.bfloat16), low_factor, preferred_element_type=jnp.float32)
    low_term = jnp.dot(proj_low.astype(jnp.bfloat16), low_factor.T, preferred_element_type=jnp.float32)
    grad_b = (-(x_dev * prec_diag[None, :] + low_term)).astype(jnp.bfloat16)
    theta_b = cur_theta.astype(jnp.bfloat16)
    gram_mat = jnp.dot(theta_b, theta_b.T, preferred_element_type=jnp.float32)
    sq_norm = jnp.sum(jnp.square(theta_b.astype(jnp.float32)), axis=1)
    sq_dist = jnp.maximum(sq_norm[:, None] + sq_norm[None, :] - 2.0 * gram_mat, 0.0)
    kern_b = jnp.exp(-sq_dist / KERN_WIDTH).astype(jnp.bfloat16)
    row_mass = jnp.sum(kern_b.astype(jnp.float32), axis=1)
    drive_term = jnp.dot(kern_b, grad_b, preferred_element_type=jnp.float32)
    pull_term = jnp.dot(kern_b, theta_b, preferred_element_type=jnp.float32)
    update_dir = (drive_term + (2.0 / KERN_WIDTH) * (row_mass[:, None] * theta_b.astype(jnp.float32) - pull_term)) / NUM_PARTICLES
    return cur_theta + STEP_SIZE * update_dir


def reference(particles, prec_diag, target_mean, low_factor):
    cur_theta = particles
    for step_idx in range(NUM_STEPS):
        cur_theta = svgd_step(cur_theta, prec_diag, target_mean, low_factor)
    return cur_theta
```

```python
import math
import jax
import jax.numpy as jnp
from jax import lax
from jax.sharding import PartitionSpec as P

NUM_STEPS = 3
F32 = jnp.float32
BF16 = jnp.bfloat16


def dot_nt(left, right):
    return lax.dot_general(left, right, (((1,), (1,)), ((), ())), preferred_element_type=F32)


def dot_nn(left, right):
    return lax.dot_general(left, right, (((1,), (0,)), ((), ())), preferred_element_type=F32)


def solution(mesh):
    part_size = mesh.shape["part"]
    feat_size = mesh.shape["feat"]
    assert part_size == 2 and feat_size == 4
    core_perm = [(0, 1), (1, 0), (2, 3), (3, 2)]
    x_perm = [(0, 2), (2, 0), (1, 3), (3, 1)]
    y_perm = [(0, 1), (1, 0)]

    def swap_core(v):
        return lax.ppermute(v, "feat", core_perm)

    def swap_x(v):
        return lax.ppermute(v, "feat", x_perm)

    def swap_y(v):
        return lax.ppermute(v, "part", y_perm)

    def local_steps(local_theta, prec_loc, mean_loc, factor_loc):
        rows_loc, feat_loc = local_theta.shape
        n_total = rows_loc * part_size
        feat_total = feat_loc * feat_size
        kern_width = 2.0 * feat_total / math.log(n_total)
        step_size = 0.15 * n_total * feat_total / math.log(n_total)
        core = lax.axis_index("feat") % 2
        half = rows_loc // 2

        def join(own, other, axis):
            return jnp.where(core == 0, jnp.concatenate([own, other], axis), jnp.concatenate([other, own], axis))

        keep = lax.dynamic_slice_in_dim(local_theta, core * half, half)
        away = lax.dynamic_slice_in_dim(local_theta, (1 - core) * half, half)
        theta = join(keep, swap_core(away), 1)
        vecs = jnp.stack([prec_loc, mean_loc])
        vecs = join(vecs, swap_core(vecs), 1)
        prec, mean = vecs[0], vecs[1]
        factor = join(factor_loc, swap_core(factor_loc), 0)

        for step_idx in range(NUM_STEPS):
            t_own = theta.astype(BF16)
            t_y = swap_y(t_own)
            t_x = swap_x(t_own)
            x_dev = theta - mean[None, :]
            z_part = lax.dot_general(factor, x_dev.astype(BF16), (((0,), (1,)), ((), ())), preferred_element_type=F32)
            s_part = jnp.sum(jnp.square(t_own.astype(F32)), axis=1)
            zs_part = jnp.concatenate([z_part, s_part[None, :]], 0)
            zs = zs_part + swap_x(zs_part)
            z_low, s_own = zs[:-1], zs[-1]
            low_term = lax.dot_general(z_low.astype(BF16), factor, (((0,), (1,)), ((), ())), preferred_element_type=F32)
            a_own = (-(x_dev * prec[None, :] + low_term)).astype(BF16)
            t_xy = swap_x(t_y)
            a_y = swap_y(a_own)
            s_y = swap_y(s_own)
            near_t = [t_own, swap_core(t_own)]
            near_x = [t_x, swap_core(t_x)]
            near_a = [a_own, swap_core(a_own)]
            near_s = [s_own, swap_core(s_own)]
            far_t = [t_y, swap_core(t_y)]
            far_x = [t_xy, swap_core(t_xy)]
            far_a = [a_y, swap_core(a_y)]
            far_s = [s_y, swap_core(s_y)]
            drive = 0.0
            pull = 0.0
            mass = 0.0
            for tb, xb, ab, sb in zip(near_t + far_t, near_x + far_x, near_a + far_a, near_s + far_s):
                gram = dot_nt(t_own, tb) + dot_nt(t_x, xb)
                sq_dist = jnp.maximum(s_own[:, None] + sb[None, :] - 2.0 * gram, 0.0)
                kern = jnp.exp(-sq_dist / kern_width).astype(BF16)
                mass = mass + jnp.sum(kern, axis=1, dtype=F32)
                drive = drive + dot_nn(kern, ab)
                pull = pull + dot_nn(kern, tb)
            update = (drive + (2.0 / kern_width) * (mass[:, None] * t_own.astype(F32) - pull)) / n_total
            theta = theta + step_size * update

        theta_own = lax.dynamic_slice_in_dim(theta, core * feat_loc, feat_loc, 1)
        theta_away = lax.dynamic_slice_in_dim(theta, (1 - core) * feat_loc, feat_loc, 1)
        return join(theta_own, swap_core(theta_away), 0)

    row_spec = P(("ens", "part"), "feat")
    vec_spec = P(("ens", "feat"))
    fac_spec = P(("ens", "feat"), None)
    return jax.shard_map(local_steps, mesh=mesh, in_specs=(row_spec, vec_spec, vec_spec, fac_spec), out_specs=row_spec, check_vma=False)
```

```python
import functools
import math
import jax
import jax.numpy as jnp
from jax import lax
from jax.experimental import pallas as pl
from jax.experimental.pallas import tpu as pltpu
from jax.sharding import PartitionSpec as P

NUM_STEPS = 3
CHUNK = 256
WIDE = 512
F32 = jnp.float32
BF16 = jnp.bfloat16
MESH = pl.DeviceIdType.MESH

OWN, SIB, FAR, FAR_SIB = 0, 1, 2, 3
(T_TO_Y, T_TO_X, T_TO_SIB, FAR_TO_X, FAR_TO_SIB, OTHER_TO_SIB, DIAG_TO_SIB,
 A_TO_Y, A_TO_SIB, FAR_A_TO_SIB, Z_TO_X) = range(11)
S_TO_SIB, S_TO_Y, FAR_S_TO_SIB = range(3)
FACTOR_TO_SIB, VECS_TO_SIB = range(2)


def dot_nt(left, right):
    return lax.dot_general(left, right, (((1,), (1,)), ((), ())), preferred_element_type=F32)


def dot_nn(left, right):
    return lax.dot_general(left, right, (((1,), (0,)), ((), ())), preferred_element_type=F32)


def dot_tn(left, right):
    return lax.dot_general(left, right, (((0,), (0,)), ((), ())), preferred_element_type=F32)


def svgd_kernel(n_total, kern_width, step_size, theta_in, vecs_in, factor_in, out, theta, vecs, factor_t,
                tb, ab, zs, sb, srow, mass, send, recv, small_send, small_recv,
                load_sem, give_sem, take_sem, table_send, table_recv):
    rows, feats = theta.shape
    wide = feats // 2
    rank = factor_t.shape[0]
    chunks = rows // CHUNK
    gain = step_size / n_total
    pull_gain = gain * 2.0 / kern_width
    feat = lax.axis_index("feat")
    part = lax.axis_index("part")
    core = lax.rem(feat, 2)
    to_sib = {"feat": feat + 1 - 2 * core}
    to_x = {"feat": lax.rem(feat + 2, 4)}
    to_y = {"part": 1 - part}
    mine = pl.ds(pl.multiple_of(core * wide, wide), wide)
    theirs = pl.ds(pl.multiple_of((1 - core) * wide, wide), wide)

    barrier = pltpu.get_barrier_semaphore()
    for peer in (to_sib, to_x, to_y):
        pl.semaphore_signal(barrier, inc=1, device_id=peer, device_id_type=MESH)

    def span(i):
        return pl.ds(pl.multiple_of(i * CHUNK, CHUNK), CHUNK)

    def half_rows(which, i):
        return pl.ds(pl.multiple_of(which * rows + i * CHUNK, CHUNK), CHUNK)

    def load(i):
        return pltpu.make_async_copy(
            theta_in.at[half_rows(core, i)], theta.at[span(i), mine], load_sem.at[0, i])

    def give(i):
        return pltpu.make_async_remote_copy(
            src_ref=theta_in.at[half_rows(1 - core, i)], dst_ref=theta.at[span(i), mine],
            send_sem=give_sem.at[0, i], recv_sem=take_sem.at[0, i], device_id=to_sib, device_id_type=MESH)

    def store(i):
        return pltpu.make_async_copy(
            theta.at[span(i), mine], out.at[half_rows(core, i)], load_sem.at[1, i])

    def give_back(i):
        return pltpu.make_async_remote_copy(
            src_ref=theta.at[span(i), theirs], dst_ref=out.at[half_rows(core, i)],
            send_sem=give_sem.at[1, i], recv_sem=take_sem.at[1, i], device_id=to_sib, device_id_type=MESH)

    def table(kind):
        src, dst = {
            FACTOR_TO_SIB: (factor_in, factor_t.at[:, mine]),
            VECS_TO_SIB: (vecs_in, vecs.at[:, mine]),
        }[kind]
        return pltpu.make_async_remote_copy(
            src_ref=src, dst_ref=dst, send_sem=table_send.at[kind], recv_sem=table_recv.at[kind],
            device_id=to_sib, device_id_type=MESH)

    def copy(kind, p, i):
        if kind == Z_TO_X:
            return pltpu.make_async_remote_copy(
                src_ref=zs.at[p, 0, :, span(i)], dst_ref=zs.at[p, 1, :, span(i)], send_sem=send.at[p, kind, i],
                recv_sem=recv.at[p, kind, i], device_id=to_x, device_id_type=MESH)
        src, dst, peer = {
            T_TO_Y: (tb.at[p, OWN, 0], tb.at[p, FAR, 0], to_y),
            T_TO_X: (tb.at[p, OWN, 0], tb.at[p, OWN, 1], to_x),
            T_TO_SIB: (tb.at[p, OWN, 0], tb.at[p, SIB, 0], to_sib),
            FAR_TO_X: (tb.at[p, FAR, 0], tb.at[p, FAR, 1], to_x),
            FAR_TO_SIB: (tb.at[p, FAR, 0], tb.at[p, FAR_SIB, 0], to_sib),
            OTHER_TO_SIB: (tb.at[p, OWN, 1], tb.at[p, SIB, 1], to_sib),
            DIAG_TO_SIB: (tb.at[p, FAR, 1], tb.at[p, FAR_SIB, 1], to_sib),
            A_TO_Y: (ab.at[p, OWN], ab.at[p, FAR], to_y),
            A_TO_SIB: (ab.at[p, OWN], ab.at[p, SIB], to_sib),
            FAR_A_TO_SIB: (ab.at[p, FAR], ab.at[p, FAR_SIB], to_sib),
        }[kind]
        return pltpu.make_async_remote_copy(
            src_ref=src.at[span(i)], dst_ref=dst.at[span(i)], send_sem=send.at[p, kind, i],
            recv_sem=recv.at[p, kind, i], device_id=peer, device_id_type=MESH)

    def small(kind, p):
        src, dst, peer = {
            S_TO_SIB: (sb.at[p, OWN], sb.at[p, SIB], to_sib),
            S_TO_Y: (sb.at[p, OWN], sb.at[p, FAR], to_y),
            FAR_S_TO_SIB: (sb.at[p, FAR], sb.at[p, FAR_SIB], to_sib),
        }[kind]
        return pltpu.make_async_remote_copy(
            src_ref=src, dst_ref=dst, send_sem=small_send.at[p, kind],
            recv_sem=small_recv.at[p, kind], device_id=peer, device_id_type=MESH)

    def each_chunk(body):
        lax.fori_loop(0, chunks, lambda i, c: (body(i), c)[1], 0)

    def emit(p, i):
        here = theta[span(i), :]
        here_b = here.astype(BF16)
        tb[p, OWN, 0, span(i), :] = here_b
        x_dev = here - vecs[1:2, :]
        near = here_b.astype(F32)
        norm = jnp.broadcast_to(jnp.sum(near * near, axis=1, keepdims=True), (CHUNK, 128))
        zs[p, 0, 0:rank, span(i)] = dot_nt(factor_t[...], x_dev.astype(BF16))
        zs[p, 0, rank:rank + 8, span(i)] = jnp.transpose(norm)[0:8, :]
        for kind in (Z_TO_X, T_TO_Y, T_TO_X, T_TO_SIB):
            copy(kind, p, i).start()

    def total_norm(p, i):
        copy(Z_TO_X, p, i).wait_recv()
        sb[p, OWN, :, span(i)] = zs[p, 0, rank:rank + 8, span(i)] + zs[p, 1, rank:rank + 8, span(i)]

    def drive(p, i):
        here = theta[span(i), :]
        z_low = zs[p, 0, 0:rank, span(i)] + zs[p, 1, 0:rank, span(i)]
        low_term = dot_tn(z_low.astype(BF16), factor_t[...])
        x_dev = here - vecs[1:2, :]
        ab[p, OWN, span(i), :] = (-(x_dev * vecs[0:1, :] + low_term)).astype(BF16)
        copy(A_TO_Y, p, i).start()
        copy(A_TO_SIB, p, i).start()

    def row_norm(p, i):
        near = tb[p, OWN, 0, span(i), :].astype(F32)
        other = tb[p, OWN, 1, span(i), :].astype(F32)
        total = jnp.sum(near * near + other * other, axis=1, keepdims=True)
        srow[span(i), :] = jnp.broadcast_to(total, (CHUNK, 128))

    def tile(p, i, blocks, start, width):
        cols = pl.ds(pl.multiple_of(start, width), width)
        parts = []
        for block in blocks:
            gram = dot_nt(tb[p, OWN, 0, span(i), :], tb[p, block, 0, cols, :])
            gram = gram + dot_nt(tb[p, OWN, 1, span(i), :], tb[p, block, 1, cols, :])
            sq_dist = jnp.maximum(srow[span(i), 0:1] + sb[p, block, 0:1, cols] - 2.0 * gram, 0.0)
            parts.append(jnp.exp(sq_dist * (-1.0 / kern_width)).astype(BF16))
        kern = jnp.concatenate(parts, axis=1)
        heavy = kern.astype(F32)
        lanes = heavy[:, 0:128]
        for q in range(1, kern.shape[1] // 128):
            lanes = lanes + heavy[:, q * 128:(q + 1) * 128]
        mass[span(i), :] += lanes
        push = dot_nn(kern, jnp.concatenate([ab[p, block, cols, :] for block in blocks], axis=0))
        pull = dot_nn(kern, jnp.concatenate([tb[p, block, 0, cols, :] for block in blocks], axis=0))
        theta[span(i), :] += gain * push - pull_gain * pull

    def near_group(p, block):
        per_row = rows // WIDE

        def body(q):
            tile(p, q // per_row, (block,), lax.rem(q, per_row) * WIDE, WIDE)
        lax.fori_loop(0, chunks * per_row, lambda q, c: (body(q), c)[1], 0)

    def far_pair(p, i, j):
        tile(p, i, (FAR, FAR_SIB), j * CHUNK, CHUNK)

    def far_arrive(p, j):
        copy(FAR_TO_X, p, j).wait_recv()
        copy(DIAG_TO_SIB, p, j).start()
        copy(A_TO_Y, p, j).wait_recv()
        copy(FAR_A_TO_SIB, p, j).start()

    def far_ready(p, j):
        copy(FAR_TO_SIB, p, j).wait_recv()
        copy(DIAG_TO_SIB, p, j).wait_recv()
        copy(FAR_A_TO_SIB, p, j).wait_recv()

    each_chunk(lambda i: load(i).start())
    vecs[:, mine] = vecs_in[...]
    factor_t[:, mine] = factor_in[...]
    pl.semaphore_wait(barrier, 3)
    for kind in (FACTOR_TO_SIB, VECS_TO_SIB):
        table(kind).start()
    each_chunk(lambda i: give(i).start())
    for kind in (FACTOR_TO_SIB, VECS_TO_SIB):
        table(kind).wait_recv()

    def begin(i):
        load(i).wait()
        give(i).wait_recv()
        emit(0, i)
    each_chunk(begin)

    def step(k, carry):
        p = lax.rem(k, 2)
        each_chunk(lambda i: total_norm(p, i))
        small(S_TO_SIB, p).start()
        small(S_TO_Y, p).start()
        each_chunk(lambda i: drive(p, i))
        mass[...] = jnp.zeros_like(mass)

        def arrive(i):
            copy(T_TO_Y, p, i).wait_recv()
            copy(FAR_TO_X, p, i).start()
            copy(FAR_TO_SIB, p, i).start()
            copy(T_TO_X, p, i).wait_recv()
            copy(OTHER_TO_SIB, p, i).start()
            row_norm(p, i)
        each_chunk(arrive)
        near_group(p, OWN)
        small(S_TO_Y, p).wait_recv()
        small(FAR_S_TO_SIB, p).start()
        far_arrive(p, 0)
        small(S_TO_SIB, p).wait_recv()

        def sib_ready(i):
            copy(T_TO_SIB, p, i).wait_recv()
            copy(OTHER_TO_SIB, p, i).wait_recv()
            copy(A_TO_SIB, p, i).wait_recv()
        each_chunk(sib_ready)
        near_group(p, SIB)
        far_arrive(p, 1)
        small(FAR_S_TO_SIB, p).wait_recv()

        def far_step(j, c):
            far_ready(p, j)
            each_chunk(lambda i: far_pair(p, i, j))

            @pl.when(j != 1)
            def _():
                far_arrive(p, 2 + j // 2)
            return c
        lax.fori_loop(0, chunks - 1, far_step, 0)
        far_ready(p, chunks - 1)

        def drain(i):
            for kind in range(11):
                copy(kind, p, i).wait_send()
        each_chunk(drain)
        for kind in range(3):
            small(kind, p).wait_send()

        def finish(i):
            far_pair(p, i, chunks - 1)
            total = jnp.sum(mass[span(i), :], axis=1, keepdims=True)
            theta[span(i), :] += pull_gain * total * tb[p, OWN, 0, span(i), :].astype(F32)

            @pl.when(k < NUM_STEPS - 1)
            def _():
                emit(1 - p, i)

            @pl.when(k == NUM_STEPS - 1)
            def _():
                store(i).start()
                give_back(i).start()
        each_chunk(finish)
        return carry
    lax.fori_loop(0, NUM_STEPS, step, 0)

    for kind in (FACTOR_TO_SIB, VECS_TO_SIB):
        table(kind).wait_send()

    def end(i):
        give(i).wait_send()
        store(i).wait()
        give_back(i).wait()
    each_chunk(end)


def solution(mesh):
    part_size = mesh.shape["part"]
    feat_size = mesh.shape["feat"]
    assert part_size == 2 and feat_size == 4

    def local_steps(local_theta, prec_loc, mean_loc, factor_loc):
        rows_loc, feat_loc = local_theta.shape
        n_total = rows_loc * part_size
        feat_total = feat_loc * feat_size
        kern_width = 2.0 * feat_total / math.log(n_total)
        step_size = 0.15 * n_total * feat_total / math.log(n_total)
        rows, feats = rows_loc // 2, feat_loc * 2
        chunks = rows // CHUNK
        assert chunks == 4
        rank = factor_loc.shape[1]
        vecs = jnp.concatenate([prec_loc[None], mean_loc[None], jnp.zeros((6, feat_loc), F32)], 0)

        vmem = pl.BlockSpec(memory_space=pltpu.VMEM)
        hbm = pl.BlockSpec(memory_space=pl.ANY)
        return pl.pallas_call(
            functools.partial(svgd_kernel, n_total, kern_width, step_size),
            out_shape=jax.ShapeDtypeStruct((rows_loc, feat_loc), F32),
            in_specs=[hbm, vmem, vmem],
            out_specs=hbm,
            scratch_shapes=[
                pltpu.VMEM((rows, feats), F32),
                pltpu.VMEM((8, feats), F32),
                pltpu.VMEM((rank, feats), BF16),
                pltpu.VMEM((2, 4, 2, rows, feats), BF16),
                pltpu.VMEM((2, 4, rows, feats), BF16),
                pltpu.VMEM((2, 2, rank + 8, rows), F32),
                pltpu.VMEM((2, 4, 8, rows), F32),
                pltpu.VMEM((rows, 128), F32),
                pltpu.VMEM((rows, 128), F32),
                pltpu.SemaphoreType.DMA((2, 11, chunks)),
                pltpu.SemaphoreType.DMA((2, 11, chunks)),
                pltpu.SemaphoreType.DMA((2, 3)),
                pltpu.SemaphoreType.DMA((2, 3)),
                pltpu.SemaphoreType.DMA((2, chunks)),
                pltpu.SemaphoreType.DMA((2, chunks)),
                pltpu.SemaphoreType.DMA((2, chunks)),
                pltpu.SemaphoreType.DMA((2,)),
                pltpu.SemaphoreType.DMA((2,)),
            ],
            compiler_params=pltpu.CompilerParams(
                collective_id=0, has_side_effects=True, vmem_limit_bytes=67043328),
            name="svgd_steps",
        )(local_theta, vecs, factor_loc.T)

    row_spec = P(("ens", "part"), "feat")
    vec_spec = P(("ens", "feat"))
    fac_spec = P(("ens", "feat"), None)
    return jax.shard_map(local_steps, mesh=mesh, in_specs=(row_spec, vec_spec, vec_spec, fac_spec), out_specs=row_spec, check_vma=False)
```

```python
import functools
import math
import jax
import jax.numpy as jnp
from jax import lax
from jax.experimental import pallas as pl
from jax.experimental.pallas import tpu as pltpu
from jax.sharding import PartitionSpec as P

NUM_STEPS = 3
CHUNK = 256
WIDE = 512
TALL = 512
F32 = jnp.float32
BF16 = jnp.bfloat16
MESH = pl.DeviceIdType.MESH

OWN, SIB, FAR, FAR_SIB = 0, 1, 2, 3
(T_TO_Y, T_TO_X, T_TO_SIB, FAR_TO_X, FAR_TO_SIB, OTHER_TO_SIB, DIAG_TO_SIB,
 A_TO_Y, A_TO_SIB, FAR_A_TO_SIB, Z_TO_X) = range(11)
S_TO_SIB, S_TO_Y, FAR_S_TO_SIB = range(3)
FACTOR_TO_SIB, VECS_TO_SIB = range(2)


def dot_nt(left, right):
    return lax.dot_general(left, right, (((1,), (1,)), ((), ())), preferred_element_type=F32)


def dot_nn(left, right):
    return lax.dot_general(left, right, (((1,), (0,)), ((), ())), preferred_element_type=F32)


def dot_tn(left, right):
    return lax.dot_general(left, right, (((0,), (0,)), ((), ())), preferred_element_type=F32)


def svgd_kernel(n_total, kern_width, step_size, theta_in, vecs_in, factor_in, out, theta, vecs, factor_t,
                tb, ab, zs, sb, srow, mass, send, recv, small_send, small_recv,
                load_sem, give_sem, take_sem, table_send, table_recv):
    rows, feats = theta.shape
    wide = feats // 2
    rank = factor_t.shape[0]
    chunks = rows // CHUNK
    gain = step_size / n_total
    pull_gain = gain * 2.0 / kern_width
    feat = lax.axis_index("feat")
    part = lax.axis_index("part")
    core = lax.rem(feat, 2)
    to_sib = {"feat": feat + 1 - 2 * core}
    to_x = {"feat": lax.rem(feat + 2, 4)}
    to_y = {"part": 1 - part}
    mine = pl.ds(pl.multiple_of(core * wide, wide), wide)
    theirs = pl.ds(pl.multiple_of((1 - core) * wide, wide), wide)

    barrier = pltpu.get_barrier_semaphore()
    for peer in (to_sib, to_x, to_y):
        pl.semaphore_signal(barrier, inc=1, device_id=peer, device_id_type=MESH)

    def span(i):
        return pl.ds(pl.multiple_of(i * CHUNK, CHUNK), CHUNK)

    def half_rows(which, i):
        return pl.ds(pl.multiple_of(which * rows + i * CHUNK, CHUNK), CHUNK)

    def load(i):
        return pltpu.make_async_copy(
            theta_in.at[half_rows(core, i)], theta.at[span(i), mine], load_sem.at[0, i])

    def give(i):
        return pltpu.make_async_remote_copy(
            src_ref=theta_in.at[half_rows(1 - core, i)], dst_ref=theta.at[span(i), mine],
            send_sem=give_sem.at[0, i], recv_sem=take_sem.at[0, i], device_id=to_sib, device_id_type=MESH)

    def store(i):
        return pltpu.make_async_copy(
            theta.at[span(i), mine], out.at[half_rows(core, i)], load_sem.at[1, i])

    def give_back(i):
        return pltpu.make_async_remote_copy(
            src_ref=theta.at[span(i), theirs], dst_ref=out.at[half_rows(core, i)],
            send_sem=give_sem.at[1, i], recv_sem=take_sem.at[1, i], device_id=to_sib, device_id_type=MESH)

    def table(kind):
        src, dst = {
            FACTOR_TO_SIB: (factor_in, factor_t.at[:, mine]),
            VECS_TO_SIB: (vecs_in, vecs.at[:, mine]),
        }[kind]
        return pltpu.make_async_remote_copy(
            src_ref=src, dst_ref=dst, send_sem=table_send.at[kind], recv_sem=table_recv.at[kind],
            device_id=to_sib, device_id_type=MESH)

    def copy(kind, p, i):
        if kind == Z_TO_X:
            return pltpu.make_async_remote_copy(
                src_ref=zs.at[p, 0, :, span(i)], dst_ref=zs.at[p, 1, :, span(i)], send_sem=send.at[p, kind, i],
                recv_sem=recv.at[p, kind, i], device_id=to_x, device_id_type=MESH)
        src, dst, peer = {
            T_TO_Y: (tb.at[p, OWN, 0], tb.at[p, FAR, 0], to_y),
            T_TO_X: (tb.at[p, OWN, 0], tb.at[p, OWN, 1], to_x),
            T_TO_SIB: (tb.at[p, OWN, 0], tb.at[p, SIB, 0], to_sib),
            FAR_TO_X: (tb.at[p, FAR, 0], tb.at[p, FAR, 1], to_x),
            FAR_TO_SIB: (tb.at[p, FAR, 0], tb.at[p, FAR_SIB, 0], to_sib),
            OTHER_TO_SIB: (tb.at[p, OWN, 1], tb.at[p, SIB, 1], to_sib),
            DIAG_TO_SIB: (tb.at[p, FAR, 1], tb.at[p, FAR_SIB, 1], to_sib),
            A_TO_Y: (ab.at[p, OWN], ab.at[p, FAR], to_y),
            A_TO_SIB: (ab.at[p, OWN], ab.at[p, SIB], to_sib),
            FAR_A_TO_SIB: (ab.at[p, FAR], ab.at[p, FAR_SIB], to_sib),
        }[kind]
        return pltpu.make_async_remote_copy(
            src_ref=src.at[span(i)], dst_ref=dst.at[span(i)], send_sem=send.at[p, kind, i],
            recv_sem=recv.at[p, kind, i], device_id=peer, device_id_type=MESH)

    def small(kind, p):
        src, dst, peer = {
            S_TO_SIB: (sb.at[p, OWN], sb.at[p, SIB], to_sib),
            S_TO_Y: (sb.at[p, OWN], sb.at[p, FAR], to_y),
            FAR_S_TO_SIB: (sb.at[p, FAR], sb.at[p, FAR_SIB], to_sib),
        }[kind]
        return pltpu.make_async_remote_copy(
            src_ref=src, dst_ref=dst, send_sem=small_send.at[p, kind],
            recv_sem=small_recv.at[p, kind], device_id=peer, device_id_type=MESH)

    def each_chunk(body):
        lax.fori_loop(0, chunks, lambda i, c: (body(i), c)[1], 0)

    def emit(p, i):
        here = theta[span(i), :]
        here_b = here.astype(BF16)
        tb[p, OWN, 0, span(i), :] = here_b
        x_dev = here - vecs[1:2, :]
        near = here_b.astype(F32)
        norm = jnp.broadcast_to(jnp.sum(near * near, axis=1, keepdims=True), (CHUNK, 128))
        zs[p, 0, 0:rank, span(i)] = dot_nt(factor_t[...], x_dev.astype(BF16))
        zs[p, 0, rank:rank + 8, span(i)] = jnp.transpose(norm)[0:8, :]
        for kind in (Z_TO_X, T_TO_Y, T_TO_X, T_TO_SIB):
            copy(kind, p, i).start()

    def total_norm(p, i):
        copy(Z_TO_X, p, i).wait_recv()
        sb[p, OWN, :, span(i)] = zs[p, 0, rank:rank + 8, span(i)] + zs[p, 1, rank:rank + 8, span(i)]

    def drive(p, i):
        here = theta[span(i), :]
        z_low = zs[p, 0, 0:rank, span(i)] + zs[p, 1, 0:rank, span(i)]
        low_term = dot_tn(z_low.astype(BF16), factor_t[...])
        x_dev = here - vecs[1:2, :]
        ab[p, OWN, span(i), :] = (-(x_dev * vecs[0:1, :] + low_term)).astype(BF16)
        copy(A_TO_Y, p, i).start()
        copy(A_TO_SIB, p, i).start()

    def row_norm(p, i):
        near = tb[p, OWN, 0, span(i), :].astype(F32)
        other = tb[p, OWN, 1, span(i), :].astype(F32)
        total = jnp.sum(near * near + other * other, axis=1, keepdims=True)
        srow[span(i), :] = jnp.broadcast_to(total, (CHUNK, 128))

    def tile(p, i, blocks, start, width, height=TALL):
        tall = pl.ds(pl.multiple_of(i * height, height), height)
        cols = pl.ds(pl.multiple_of(start, width), width)
        parts = []
        for block in blocks:
            gram = dot_nt(tb[p, OWN, 0, tall, :], tb[p, block, 0, cols, :])
            gram = gram + dot_nt(tb[p, OWN, 1, tall, :], tb[p, block, 1, cols, :])
            sq_dist = jnp.maximum(srow[tall, 0:1] + sb[p, block, 0:1, cols] - 2.0 * gram, 0.0)
            parts.append(jnp.exp(sq_dist * (-1.0 / kern_width)).astype(BF16))
        kern = jnp.concatenate(parts, axis=1)
        heavy = kern.astype(F32)
        lanes = heavy[:, 0:128]
        for q in range(1, kern.shape[1] // 128):
            lanes = lanes + heavy[:, q * 128:(q + 1) * 128]
        mass[tall, :] += lanes
        push = dot_nn(kern, jnp.concatenate([ab[p, block, cols, :] for block in blocks], axis=0))
        pull = dot_nn(kern, jnp.concatenate([tb[p, block, 0, cols, :] for block in blocks], axis=0))
        theta[tall, :] += gain * push - pull_gain * pull

    def near_group(p, block, first, last):
        per_row = rows // WIDE

        def body(q):
            tile(p, q // per_row, (block,), lax.rem(q, per_row) * WIDE, WIDE)
        lax.fori_loop(first, last, lambda q, c: (body(q), c)[1], 0)

    def far_pair(p, i, j):
        tile(p, i, (FAR, FAR_SIB), j * CHUNK, CHUNK)

    def far_arrive(p, j):
        copy(FAR_TO_X, p, j).wait_recv()
        copy(DIAG_TO_SIB, p, j).start()
        copy(A_TO_Y, p, j).wait_recv()
        copy(FAR_A_TO_SIB, p, j).start()

    def far_ready(p, j):
        copy(FAR_TO_SIB, p, j).wait_recv()
        copy(DIAG_TO_SIB, p, j).wait_recv()
        copy(FAR_A_TO_SIB, p, j).wait_recv()

    each_chunk(lambda i: load(i).start())
    vecs[:, mine] = vecs_in[...]
    factor_t[:, mine] = factor_in[...]
    pl.semaphore_wait(barrier, 3)
    for kind in (FACTOR_TO_SIB, VECS_TO_SIB):
        table(kind).start()
    each_chunk(lambda i: give(i).start())
    for kind in (FACTOR_TO_SIB, VECS_TO_SIB):
        table(kind).wait_recv()

    def begin(i):
        load(i).wait()
        give(i).wait_recv()
        emit(0, i)
    each_chunk(begin)

    def step(k, carry):
        p = lax.rem(k, 2)
        near_tiles = (rows // TALL) * (rows // WIDE)
        each_chunk(lambda i: total_norm(p, i))
        small(S_TO_SIB, p).start()
        small(S_TO_Y, p).start()
        each_chunk(lambda i: drive(p, i))
        mass[...] = jnp.zeros_like(mass)

        def arrive(i):
            copy(T_TO_Y, p, i).wait_recv()
            copy(FAR_TO_X, p, i).start()
            copy(FAR_TO_SIB, p, i).start()
            copy(T_TO_X, p, i).wait_recv()
            copy(OTHER_TO_SIB, p, i).start()
            row_norm(p, i)

            @pl.when(i == 1)
            def _():
                near_group(p, OWN, 0, 1)
        each_chunk(arrive)
        near_group(p, OWN, 1, near_tiles)
        small(S_TO_Y, p).wait_recv()
        small(FAR_S_TO_SIB, p).start()
        far_arrive(p, 0)
        small(S_TO_SIB, p).wait_recv()

        def sib_ready(i):
            copy(T_TO_SIB, p, i).wait_recv()
            copy(OTHER_TO_SIB, p, i).wait_recv()
            copy(A_TO_SIB, p, i).wait_recv()
        each_chunk(sib_ready)
        near_group(p, SIB, 0, near_tiles)
        far_arrive(p, 1)
        small(FAR_S_TO_SIB, p).wait_recv()

        def far_step(j, c):
            far_ready(p, j)
            lax.fori_loop(0, rows // TALL, lambda i, d: (far_pair(p, i, j), d)[1], 0)

            @pl.when(j != 1)
            def _():
                far_arrive(p, 2 + j // 2)
            return c
        lax.fori_loop(0, chunks - 1, far_step, 0)
        far_ready(p, chunks - 1)

        def drain(i):
            for kind in range(11):
                copy(kind, p, i).wait_send()
        each_chunk(drain)
        for kind in range(3):
            small(kind, p).wait_send()

        def finish(i):
            tile(p, i, (FAR, FAR_SIB), (chunks - 1) * CHUNK, CHUNK, CHUNK)
            total = jnp.sum(mass[span(i), :], axis=1, keepdims=True)
            theta[span(i), :] += pull_gain * total * tb[p, OWN, 0, span(i), :].astype(F32)

            @pl.when(k < NUM_STEPS - 1)
            def _():
                emit(1 - p, i)

            @pl.when(k == NUM_STEPS - 1)
            def _():
                store(i).start()
                give_back(i).start()
        each_chunk(finish)
        return carry
    lax.fori_loop(0, NUM_STEPS, step, 0)

    for kind in (FACTOR_TO_SIB, VECS_TO_SIB):
        table(kind).wait_send()

    def end(i):
        give(i).wait_send()
        store(i).wait()
        give_back(i).wait()
    each_chunk(end)


def solution(mesh):
    part_size = mesh.shape["part"]
    feat_size = mesh.shape["feat"]
    assert part_size == 2 and feat_size == 4

    def local_steps(local_theta, prec_loc, mean_loc, factor_loc):
        rows_loc, feat_loc = local_theta.shape
        n_total = rows_loc * part_size
        feat_total = feat_loc * feat_size
        kern_width = 2.0 * feat_total / math.log(n_total)
        step_size = 0.15 * n_total * feat_total / math.log(n_total)
        rows, feats = rows_loc // 2, feat_loc * 2
        chunks = rows // CHUNK
        assert chunks == 4
        rank = factor_loc.shape[1]
        vecs = jnp.concatenate([prec_loc[None], mean_loc[None], jnp.zeros((6, feat_loc), F32)], 0)

        vmem = pl.BlockSpec(memory_space=pltpu.VMEM)
        hbm = pl.BlockSpec(memory_space=pl.ANY)
        return pl.pallas_call(
            functools.partial(svgd_kernel, n_total, kern_width, step_size),
            out_shape=jax.ShapeDtypeStruct((rows_loc, feat_loc), F32),
            in_specs=[hbm, vmem, vmem],
            out_specs=hbm,
            scratch_shapes=[
                pltpu.VMEM((rows, feats), F32),
                pltpu.VMEM((8, feats), F32),
                pltpu.VMEM((rank, feats), BF16),
                pltpu.VMEM((2, 4, 2, rows, feats), BF16),
                pltpu.VMEM((2, 4, rows, feats), BF16),
                pltpu.VMEM((2, 2, rank + 8, rows), F32),
                pltpu.VMEM((2, 4, 8, rows), F32),
                pltpu.VMEM((rows, 128), F32),
                pltpu.VMEM((rows, 128), F32),
                pltpu.SemaphoreType.DMA((2, 11, chunks)),
                pltpu.SemaphoreType.DMA((2, 11, chunks)),
                pltpu.SemaphoreType.DMA((2, 3)),
                pltpu.SemaphoreType.DMA((2, 3)),
                pltpu.SemaphoreType.DMA((2, chunks)),
                pltpu.SemaphoreType.DMA((2, chunks)),
                pltpu.SemaphoreType.DMA((2, chunks)),
                pltpu.SemaphoreType.DMA((2,)),
                pltpu.SemaphoreType.DMA((2,)),
            ],
            compiler_params=pltpu.CompilerParams(
                collective_id=0, has_side_effects=True, vmem_limit_bytes=67043328),
            name="svgd_steps",
        )(local_theta, vecs, factor_loc.T)

    row_spec = P(("ens", "part"), "feat")
    vec_spec = P(("ens", "feat"))
    fac_spec = P(("ens", "feat"), None)
    return jax.shard_map(local_steps, mesh=mesh, in_specs=(row_spec, vec_spec, vec_spec, fac_spec), out_specs=row_spec, check_vma=False)
```
